32 devices in a mesh: blk: 8 (over y, x, core), grp: 4 (over z).
Axes of the slice: x: 2, y: 2, z: 4, core: 2. Of those that a mesh axis runs over, the one named last changes fastest.
Arguments:
- source: float32 [2048, 128], P(('blk', 'grp')), may hold values from -3 to 3
- target: float32 [2048, 128], P(('blk', 'grp')), may hold values from -3 to 3
- source_mass: float32 [2048], P(('blk', 'grp')), may hold values from 0.25 to 4
- target_mass: float32 [2048], P(('blk', 'grp')), may hold values from 0.25 to 4
Outputs:
- source_dual: float32 [2048], P(('blk', 'grp'))
- target_dual: float32 [2048], P(('blk', 'grp'))
The draws below stay inside these ranges and needn't reach their ends.
All inputs are finite; a program needn't handle non-finite values.
Results may differ from the reference program's by a relative error of at most 0.0003.
Values sent between devices are 32-bit elements; how exact they have to be, the bound alone decides.
A program may use at most 64 MiB of HBM per device.

```python
import math
import jax
import jax.numpy as jnp
from jax import lax

D = 128
ITERS = 8
POINTS = 2048


def cloud_parts(key):
    cluster_count = max(POINTS // 64, 1)
    centres = jax.random.normal(jax.random.fold_in(key, 3), (cluster_count, D), jnp.float32)
    member = jax.random.randint(jax.random.fold_in(key, 5), (POINTS,), 0, cluster_count)
    spread = jax.random.normal(jax.random.fold_in(key, 7), (POINTS, D), jnp.float32)
    base = 0.11 * centres[member] + 0.1 * spread
    order = jax.random.permutation(jax.random.fold_in(key, 9), POINTS)
    return (base, order)


def far_shift(key):
    picked_count = max(POINTS // 256, 2)
    picks = jax.random.permutation(jax.random.fold_in(key, 19), POINTS)[:picked_count]
    strength = jax.random.uniform(jax.random.fold_in(key, 23), (picked_count,), jnp.float32, 0.85, 1.25)
    flags = jnp.zeros((POINTS,), jnp.float32).at[picks].set(strength)
    return (110.0 / D) ** 0.5 * flags[:, None]


def draw_source(key, part):
    base, order = cloud_parts(key)
    noise = 0.05 * jax.random.normal(jax.random.fold_in(key, 11), (POINTS, D), jnp.float32)
    points = base + noise
    points = points + far_shift(key)
    return jnp.clip(points, -3.0, 3.0)


def draw_target(key, part):
    base, order = cloud_parts(key)
    matched = base[order]
    noise = 0.05 * jax.random.normal(jax.random.fold_in(key, 13), (POINTS, D), jnp.float32)
    return jnp.clip(matched + noise, -3.0, 3.0)


def levels(key, dims, pieces, least, top_value):
    level, own = 1.0, jax.random.fold_in(key, 6)
    for dim, shards_of in pieces:
        heights = jnp.exp(jax.random.uniform(jax.random.fold_in(own, dim), (shards_of,), jnp.float32, least / len(pieces), top_value / len(pieces)))
        level = level * jnp.repeat(heights, dims[dim] // shards_of).reshape([-1 if axis == dim else 1 for axis in range(len(dims))])
    return level


def setup_inputs(seed: int = 0) -> dict:
    key_of = jax.random.split(jax.random.key(seed), 5)
    source = draw_source(jax.random.fold_in(key_of[4], 71), 0)
    target = draw_target(jax.random.fold_in(key_of[4], 71), 0)
    source_mass = jnp.clip(jnp.exp(math.log(4.0) - 2.7725887 * jax.random.uniform(key_of[2], (POINTS,), jnp.float32) ** levels(key_of[2], (POINTS,), ((0, 32),), -0.2, 0.2)), 0.25, 4.0)
    target_mass = jnp.clip(jnp.exp(math.log(4.0) - 2.7725887 * jax.random.uniform(key_of[3], (POINTS,), jnp.float32) ** levels(key_of[3], (POINTS,), ((0, 32),), -0.2, 0.2)), 0.25, 4.0)
    return {"source": source, "target": target, "source_mass": source_mass, "target_mass": target_mass}


eps = 0.5


def half_step(rows, cols, col_dual, col_logmass):
    total = rows.shape[0]
    width = rows.shape[1]
    block = math.gcd(total, 1024)
    col_sq = jnp.sum(cols * cols, axis=1)

    def one_block(piece):
        row_sq = jnp.sum(piece * piece, axis=1)
        inner = lax.dot_general(piece, cols, (((1,), (1,)), ((), ())), precision=lax.Precision.HIGHEST, preferred_element_type=jnp.float32)
        cost = row_sq[:, None] + col_sq[None, :] - 2.0 * inner
        score = col_logmass[None, :] + (col_dual[None, :] - cost) / eps
        top = jnp.max(score, axis=1)
        total_exp = jnp.sum(jnp.exp(score - top[:, None]), axis=1)
        return -eps * (top + jnp.log(total_exp))

    return lax.map(one_block, rows.reshape(total // block, block, width)).reshape(total)


def reference(source, target, source_mass, target_mass):
    log_source = jnp.log(source_mass)
    log_target = jnp.log(target_mass)
    target_dual = jnp.zeros((target.shape[0],), jnp.float32)
    source_dual = jnp.zeros((source.shape[0],), jnp.float32)
    for step in range(ITERS):
        source_dual = half_step(source, target, target_dual, log_target)
        target_dual = half_step(target, source, source_dual, log_source)
    return source_dual, target_dual
```

```python
import functools
import math

import jax
import jax.numpy as jnp
from jax import lax
from jax.experimental import pallas as pl
from jax.experimental.pallas import tpu as pltpu
from jax.sharding import PartitionSpec as P

ITERS = 8
eps = 0.5
LOG2E = math.log2(math.e)
ALPHA = LOG2E / eps
LANES = 128
SUB = 8
OCT = 8
PIECES = 2
UNIT = 4
GROUPS = 32
MESH = pl.DeviceIdType.MESH
BUDGET = 36 * 2**20


def exp2(x):
    return jnp.exp2(x)


def log2(x):
    return jnp.log2(x)


def lse_blocks(pairs):
    top = functools.reduce(jnp.maximum, [m for m, _ in pairs])
    if len(pairs) == 1:
        return pairs[0]
    return top, sum(s * exp2(m - top) for m, s in pairs)


def wide_kernel(blk_n, grp_n, part, count, pieces, src_ref, tgt_ref, smass_ref, tmass_ref, out_ref,
           src_all, tgt_all, spack, tpack, cost, tcat, u, v, loga, logb, part_lse, piece_top, piece_sum,
           s_send, f_send, s_recv, t_send, t_recv, x_send, x_recv):
    n_dev = blk_n * grp_n
    rep = LANES // count
    chunks = n_dev // rep
    quads = blk_n // part
    t_dev = quads * grp_n
    nj = t_dev * count
    b, g = lax.axis_index("blk"), lax.axis_index("grp")
    me = b * grp_n + g
    q, p = b // part, b % part
    mine_t = q * grp_n + g

    peers = n_dev // OCT
    z, low = (b // OCT) * grp_n + g, b % OCT

    def flip(i, bit):
        return i + bit * (1 - 2 * ((i // bit) % 2))

    def place(step, bits):
        peer = lax.rem(z + step, peers)
        home = low
        for bit in (1, 2, 4):
            if bits & bit:
                home = flip(home, bit)
        return ((peer // grp_n) * OCT + home) * grp_n + peer % grp_n

    barrier = pltpu.get_barrier_semaphore()

    def greet(step, _):
        other = place(step, 0)
        pl.semaphore_signal(barrier, inc=1, device_id=(other // grp_n, other % grp_n), device_id_type=MESH)
        return 0

    lax.fori_loop(1, peers, greet, 0)

    def greet_part(step, _):
        other = q * part + lax.rem(p + step, part)
        pl.semaphore_signal(barrier, inc=1, device_id=(other, g), device_id_type=MESH)
        return 0

    lax.fori_loop(1, part, greet_part, 0)

    lane = lax.broadcasted_iota(jnp.int32, (1, LANES), 1)
    here = lane // count == me % rep

    def pack(ref, mass_ref, out, scale):
        out[0:count, :] = ref[...] * scale
        row = log2(mass_ref[...])
        row = jnp.where(here, jnp.concatenate([row] * rep, axis=1), 0.0)
        out[count : count + SUB, :] = jnp.broadcast_to(row, (SUB, LANES))

    pack(src_ref, smass_ref, spack, 2.0 * ALPHA)
    pack(tgt_ref, tmass_ref, tpack, 1.0)
    src_all[pl.ds(me, 1)] = spack[...][None]
    tgt_all[pl.ds(mine_t, 1)] = tpack[...][None]
    pl.semaphore_wait(barrier, peers + part - 2)

    def tgt_copy(slot, r, sem_slot):
        return pltpu.make_async_remote_copy(
            src_ref=tpack, dst_ref=tgt_all.at[slot],
            send_sem=t_send.at[r], recv_sem=t_recv.at[sem_slot],
            device_id=((r // grp_n) * part + p, r % grp_n), device_id_type=MESH)

    def src_copy(slot, d, step):
        return pltpu.make_async_remote_copy(
            src_ref=spack, dst_ref=src_all.at[slot],
            send_sem=s_send.at[step], recv_sem=s_recv.at[slot],
            device_id=(d // grp_n, d % grp_n), device_id_type=MESH)

    def push(slot, way):
        return pltpu.make_async_remote_copy(
            src_ref=src_all.at[slot], dst_ref=src_all.at[slot],
            send_sem=f_send.at[way, slot], recv_sem=s_recv.at[slot],
            device_id=(flip(b, 2 ** way), g), device_id_type=MESH)

    def arrive(slot):
        src_copy(slot, me, 0).wait_recv()

    def send_t(step, _):
        tgt_copy(mine_t, lax.rem(mine_t + step, t_dev), mine_t).start()
        return 0

    def send_s(step, _):
        src_copy(me, place(step, 0), step).start()
        return 0

    def wait_t(step, _):
        r = lax.rem(mine_t + step, t_dev)
        tgt_copy(mine_t, r, mine_t).wait_send()
        tgt_copy(r, r, r).wait_recv()
        return 0

    def make_cost(k):
        blocks = [src_all[k * rep + i, 0:count, :] for i in range(rep)]
        masses = sum(src_all[k * rep + i, count : count + 1, :] for i in range(rep))
        loga[pl.ds(k, 1), :] = masses
        cost[k] = lax.dot_general(
            tcat[...], jnp.concatenate(blocks, axis=0), (((1,), (1,)), ((), ())),
            precision=lax.Precision.HIGHEST, preferred_element_type=jnp.float32)

    def costs(bits):
        home = low
        for bit in (1, 2, 4):
            if bits & bit:
                home = flip(home, bit)
        per = grp_n // rep

        def one(i, _):
            make_cost(((i // per) * OCT + home) * per + i % per)
            return 0

        lax.fori_loop(0, peers // rep, one, 0)

    for way in range(3):
        push(me, way).start()
    lax.fori_loop(1, peers, send_s, 0)
    lax.fori_loop(1, t_dev, send_t, 0)

    def relay(bits, ways):
        def go(step, _):
            slot = place(step, bits)
            arrive(slot)
            for way in ways:
                push(slot, way).start()
            return 0
        return go

    half = peers // 2
    lax.fori_loop(1, peers, relay(0, (1, 2, 0)), 0)
    lax.fori_loop(1, t_dev, wait_t, 0)

    eye = (lax.broadcasted_iota(jnp.int32, (count, LANES), 1) % count
           == lax.broadcasted_iota(jnp.int32, (count, LANES), 0))
    for r in range(t_dev):
        rows = slice(r * count, (r + 1) * count)
        block = tgt_all[r, 0:count, :]
        tcat[rows, :] = block
        mass = jnp.sum(jnp.where(eye, tgt_all[r, count : count + 1, :], 0.0), axis=1, keepdims=True)
        square = jnp.sum(block * block, axis=1, keepdims=True)
        logb[rows, :] = jnp.broadcast_to(mass, (count, LANES))
        u[rows, :] = jnp.broadcast_to(mass - ALPHA * square, (count, LANES))

    lax.fori_loop(0, half, relay(2, (2, 0)), 0)
    lax.fori_loop(0, half, relay(4, (0,)), 0)
    lax.fori_loop(half, peers, relay(4, (1, 0)), 0)
    lax.fori_loop(half, peers, relay(2, (0,)), 0)
    costs(0)
    costs(2)
    costs(4)
    lax.fori_loop(0, peers, relay(6, (0,)), 0)
    costs(6)
    for bits in (1, 3, 5, 7):
        lax.fori_loop(0, peers, relay(bits, ()), 0)
        costs(bits)

    def sent_s(step, _):
        src_copy(me, place(step, 0), step).wait_send()
        return 0

    def sent(bits, ways):
        def go(step, _):
            for way in ways:
                push(place(step, bits), way).wait_send()
            return 0
        return go

    lax.fori_loop(1, peers, sent_s, 0)
    lax.fori_loop(0, peers, sent(0, (0, 1, 2)), 0)
    lax.fori_loop(0, half, sent(2, (2, 0)), 0)
    lax.fori_loop(0, half, sent(4, (0,)), 0)
    lax.fori_loop(half, peers, sent(4, (1, 0)), 0)
    lax.fori_loop(half, peers, sent(2, (0,)), 0)
    lax.fori_loop(0, peers, sent(6, (0,)), 0)

    rows_at_once = min(nj, 128)
    size = chunks // pieces
    unit = math.gcd(size, UNIT)

    def source_unit(slot, c, k0):
        tops, totals = [], []
        for h in range(unit):
            pairs = []
            for r in range(0, nj, rows_at_once):
                x = cost[c * size + k0 + h, r : r + rows_at_once, :] + u[r : r + rows_at_once, :]
                x = x.reshape(rows_at_once // SUB, SUB, LANES)
                m = jnp.max(x, axis=0)
                pairs.append((m, jnp.sum(exp2(x - m[None]), axis=0)))
            m, s = lse_blocks(pairs)
            top = jnp.max(m, axis=0, keepdims=True)
            tops.append(top)
            totals.append(jnp.sum(s * exp2(m - top), axis=0, keepdims=True))
        part_lse[slot, c, p, pl.ds(k0, unit), :] = (
            jnp.concatenate(tops, axis=0) + log2(jnp.concatenate(totals, axis=0)))

    groups = math.gcd(nj // SUB, GROUPS)

    def target_rows(c, i):
        for h in range(groups):
            rows = pl.ds(pl.multiple_of((i * groups + h) * SUB, SUB), SUB)
            pairs = []
            for k0 in range(c * size, (c + 1) * size, 16):
                x = [cost[k, rows, :] + v[k : k + 1, :] for k in range(k0, min(k0 + 16, (c + 1) * size))]
                m = functools.reduce(jnp.maximum, x)
                pairs.append((m, sum(exp2(y - m) for y in x)))
            m, s = lse_blocks(pairs)
            if c < pieces - 1:
                piece_top[c, rows, :] = m
                piece_sum[c, rows, :] = s
                continue
            m, s = lse_blocks([(m, s)] + [(piece_top[i2, rows, :], piece_sum[i2, rows, :]) for i2 in range(c)])
            top = jnp.max(m, axis=1, keepdims=True)
            total = jnp.sum(s * exp2(m - top), axis=1, keepdims=True)
            u[rows, :] = logb[rows, :] - (top + log2(total))

    def swap(slot, c, writer, other, sem_at):
        return pltpu.make_async_remote_copy(
            src_ref=part_lse.at[slot, c, p], dst_ref=part_lse.at[slot, c, writer],
            send_sem=x_send.at[slot, c, other], recv_sem=x_recv.at[slot, c, sem_at],
            device_id=(q * part + other, g), device_id_type=MESH)

    def iteration(t, _):
        slot = lax.rem(t, 2)

        for c in range(pieces):
            def one(i, _):
                source_unit(slot, c, i * unit)
                return 0

            if size == unit:
                source_unit(slot, c, 0)
            else:
                lax.fori_loop(0, size // unit, one, 0)
            for step in range(1, part):
                swap(slot, c, p, lax.rem(p + step, part), p).start()
        for c in range(pieces):
            for step in range(1, part):
                other = lax.rem(p + step, part)
                swap(slot, c, other, other, other).wait_recv()
            parts = [part_lse[slot, c, i] for i in range(part)]
            top = functools.reduce(jnp.maximum, parts)
            rows = slice(c * size, (c + 1) * size)
            v[rows, :] = loga[rows, :] - (top + log2(sum(exp2(y - top) for y in parts)))

            def two(i, _):
                target_rows(c, i)
                return 0

            lax.fori_loop(0, nj // (SUB * groups), two, 0)
        for c in range(pieces):
            for step in range(1, part):
                swap(slot, c, p, lax.rem(p + step, part), p).wait_send()
        return 0

    lax.fori_loop(0, ITERS, iteration, 0)

    def to_lanes(column):
        return jnp.sum(jnp.where(eye, column, 0.0), axis=0, keepdims=True)

    src = src_ref[...]
    row = pl.ds(me // rep, 1)
    lse_s = loga[row, :] - v[row, :]
    first = to_lanes(jnp.sum(src * src, axis=1, keepdims=True)) - (1.0 / ALPHA) * lse_s
    tgt = tgt_ref[...]
    own = pl.ds(pl.multiple_of(mine_t * count, count), count)
    lse_t = logb[own, :] - u[own, :]
    second = to_lanes(jnp.sum(tgt * tgt, axis=1, keepdims=True) - (1.0 / ALPHA) * lse_t)
    picked = first[:, 0:count]
    for i in range(1, rep):
        picked = jnp.where(me % rep == i, first[:, i * count : (i + 1) * count], picked)
    out_ref[0:1, 0:count] = picked
    out_ref[1:2, 0:count] = second[:, 0:count]


FLOOR = 2.0**-40
GROUP = 8
MROWS = 256


def split(x):
    hi = x.astype(jnp.bfloat16)
    return hi, (x - hi.astype(jnp.float32)).astype(jnp.bfloat16)


def xor(x, y):
    return sum(((x // bit + y // bit) % 2) * bit for bit in (1, 2, 4))


def mix(z, step, peers):
    other = 0
    bit = 1
    while bit < peers:
        other = other + ((z // bit + step // bit) % 2) * bit
        bit *= 2
    return other


def chip_kernel(grp_n, count, src_ref, tgt_ref, smass_ref, tmass_ref, out_ref, src_hbm, tgt_hbm,
                src_all, tgt_all, spack, tpack, tcat, expo, bvec, cvec, own, msg, msg_in,
                part, part_in, rho, mass_a, scale, tops,
                s_send, f_send, s_recv, t_send, g_send, t_recv, m_send, m_recv, x_send, x_recv, h_sem):
    wide = count + 1
    lines = OCT // 2
    slots_t = lines * grp_n
    nt = slots_t * count
    groups = nt // SUB
    width = grp_n * count
    halves = width // LANES
    rep = LANES // count
    chunks = OCT * halves
    b, g = lax.axis_index("blk"), lax.axis_index("grp")
    me = b * grp_n + g
    core = b % 2
    mate = b + 1 - 2 * core

    def side(bits):
        return xor(b, bits)

    def slot_of(home, z):
        return home * grp_n + z

    barrier = pltpu.get_barrier_semaphore()

    def greet(step, _):
        pl.semaphore_signal(barrier, inc=1, device_id=(b, mix(g, step, grp_n)), device_id_type=MESH)
        return 0

    lax.fori_loop(1, grp_n, greet, 0)
    for bits in (1, 2, 4):
        pl.semaphore_signal(barrier, inc=1, device_id=(side(bits), g), device_id_type=MESH)

    lane = lax.broadcasted_iota(jnp.int32, (1, LANES), 1)

    def pack(ref, mass_ref, out, place):
        out[0:count, :] = ref[...]
        row = jnp.concatenate([mass_ref[...]] * rep, axis=1)
        out[count:wide, :] = jnp.where(lane // count == place, row, 0.0)

    pack(src_ref, smass_ref, spack, me % rep)
    pack(tgt_ref, tmass_ref, tpack, 0)
    src_all[pl.ds(me, 1)] = spack[...][None]
    tgt_all[pl.ds(me, 1)] = tpack[...][None]
    pl.semaphore_wait(barrier, grp_n + 2)

    def line(pk, buf, send, recv, step):
        return pltpu.make_async_remote_copy(
            src_ref=pk, dst_ref=buf.at[me], send_sem=send.at[step], recv_sem=recv.at[me],
            device_id=(b, mix(g, step, grp_n)), device_id_type=MESH)

    def push(buf, send, recv, slot, way):
        return pltpu.make_async_remote_copy(
            src_ref=buf.at[slot], dst_ref=buf.at[slot], send_sem=send.at[way, slot], recv_sem=recv.at[slot],
            device_id=(side(2 ** way), g), device_id_type=MESH)

    def first(pk, buf, send, recv, way):
        return pltpu.make_async_remote_copy(
            src_ref=pk, dst_ref=buf.at[me], send_sem=send.at[way, me], recv_sem=recv.at[me],
            device_id=(side(2 ** way), g), device_id_type=MESH)

    def s_push(slot, way):
        return push(src_all, f_send, s_recv, slot, way)

    def t_push(slot, way):
        return push(tgt_all, g_send, t_recv, slot, way)

    def s_arrive(slot):
        s_push(slot, 0).wait_recv()

    def t_arrive(slot):
        t_push(slot, 0).wait_recv()

    for way in (1, 2):
        first(tpack, tgt_all, g_send, t_recv, way).start()

    def send_line(pk, buf, send, recv):
        def go(step, _):
            line(pk, buf, send, recv, step).start()
            return 0
        lax.fori_loop(1, grp_n, go, 0)

    send_line(tpack, tgt_all, t_send, t_recv)
    for way in (1, 2, 0):
        first(spack, src_all, f_send, s_recv, way).start()
    send_line(spack, src_all, s_send, s_recv)

    def relay(pushes, arrive, bits, ways, lo, hi):
        def go(step, _):
            slot = slot_of(side(bits), mix(g, step, grp_n))
            arrive(slot)
            for way in ways:
                pushes(slot, way).start()
            return 0
        lax.fori_loop(lo, hi, go, 0)

    eye = (lax.broadcasted_iota(jnp.int32, (count, LANES), 1)
           == lax.broadcasted_iota(jnp.int32, (count, LANES), 0))

    def prepare(bits):
        home = side(bits)
        for z in range(grp_n):
            slot = slot_of(home, z)
            rows = pl.ds(pl.multiple_of(((home // 2) * grp_n + z) * count, count), count)
            block = tgt_all[slot, 0:count, :]
            hi, lo = split(block)
            tcat[rows, 0:LANES] = hi
            tcat[rows, LANES : 2 * LANES] = lo
            mass = jnp.sum(jnp.where(eye, tgt_all[slot, count:wide, :], 0.0), axis=1, keepdims=True)
            square = jnp.sum(block * block, axis=1, keepdims=True)
            mass = jnp.broadcast_to(mass, (count, LANES))
            bvec[rows, :] = mass
            cvec[rows, :] = log2(mass) - ALPHA * square

    half = grp_n // 2
    relay(t_push, t_arrive, 0, (1, 2), 1, grp_n)
    relay(s_push, s_arrive, 0, (1, 2, 0), 1, grp_n)
    prepare(0)
    relay(t_push, t_arrive, 2, (2,), 0, half)
    relay(t_push, t_arrive, 4, (), 0, half)
    relay(t_push, t_arrive, 4, (1,), half, grp_n)
    relay(t_push, t_arrive, 2, (), half, grp_n)
    relay(s_push, s_arrive, 2, (2, 0), 0, half)
    relay(s_push, s_arrive, 4, (0,), 0, half)
    relay(s_push, s_arrive, 4, (1, 0), half, grp_n)
    relay(s_push, s_arrive, 2, (0,), half, grp_n)
    prepare(2)
    prepare(4)
    relay(t_push, t_arrive, 6, (), 0, grp_n)
    prepare(6)

    def tell(kb):
        return pltpu.make_async_remote_copy(
            src_ref=msg.at[kb], dst_ref=msg_in.at[kb], send_sem=m_send.at[kb], recv_sem=m_recv.at[kb],
            device_id=(mate, g), device_id_type=MESH)

    def build(kb):
        s = jnp.concatenate([src_all[kb * grp_n + z, 0:count, :] for z in range(grp_n)], axis=0) * (2.0 * ALPHA)
        hi, lo = split(s)
        twice = jnp.concatenate([hi, hi], axis=1)
        dims = (((1,), (1,)), ((), ()))
        top = None
        for r in range(0, nt, MROWS):
            x = (lax.dot_general(tcat[r : r + MROWS, :], twice, dims, preferred_element_type=jnp.float32)
                 + lax.dot_general(tcat[r : r + MROWS, 0:LANES], lo, dims, preferred_element_type=jnp.float32))
            c = cvec[r : r + MROWS, :].reshape(MROWS // SUB, SUB, LANES)
            tall = []
            for h in range(halves):
                y = x[:, h * LANES : (h + 1) * LANES].reshape(MROWS // SUB, SUB, LANES) + c
                expo[r // SUB : (r + MROWS) // SUB, kb * halves + h] = y
                tall.append(jnp.max(y, axis=0))
            top = tall if top is None else [jnp.maximum(p, q) for p, q in zip(top, tall)]
        for h in range(halves):
            m = jnp.max(top[h], axis=0, keepdims=True)
            total = jnp.zeros((SUB, LANES), jnp.float32)
            for r in range(0, nt, MROWS):
                at = slice(r // SUB, (r + MROWS) // SUB)
                y = exp2(expo[at, kb * halves + h] - m[None])
                expo[at, kb * halves + h] = y
                total = total + jnp.sum(y, axis=0)
            msg[kb, h : h + 1, :] = m
            msg[kb, halves + h : halves + h + 1, :] = jnp.sum(total, axis=0, keepdims=True)
            mass = sum(src_all[kb * grp_n + h * rep + i, count:wide, :] for i in range(rep))
            mass_a[pl.ds(kb * halves + h, 1), :] = mass
        tell(kb).start()

    def even(i, _):
        build(side(2 * i))
        return 0

    def odd(i, _):
        home = side(2 * i + 1)

        def go(z, _):
            s_arrive(slot_of(home, z))
            return 0

        lax.fori_loop(0, grp_n, go, 0)
        build(home)
        return 0

    lax.fori_loop(0, 3, even, 0)
    relay(s_push, s_arrive, 6, (0,), 0, grp_n)
    lax.fori_loop(3, 4, even, 0)
    lax.fori_loop(0, 4, odd, 0)

    def hand(i, _):
        t_push(slot_of(2 * (i // grp_n) + core, i % grp_n), 0).start()
        return 0

    lax.fori_loop(0, slots_t, hand, 0)
    copy_s = pltpu.make_async_copy(src_all, src_hbm, h_sem.at[0])
    copy_s.start()

    def told(kb, _):
        tell(kb).wait()
        rows = pl.ds(kb * halves, halves)
        m, s = msg[kb, 0:halves, :], msg[kb, halves : 2 * halves, :]
        m2, s2 = msg_in[kb, 0:halves, :], msg_in[kb, halves : 2 * halves, :]
        top = jnp.maximum(m, m2)
        q = exp2(m - top)
        total = q * s + exp2(m2 - top) * s2
        tops[rows, :] = top
        scale[rows, :] = q
        rho[rows, :] = q * (mass_a[rows, :] / total)
        return 0

    lax.fori_loop(0, OCT, told, 0)

    def row_sum(r, weights):
        terms = [expo[r, k] * weights[k] for k in range(chunks)]
        while len(terms) > 1:
            terms = [p + q for p, q in zip(terms[::2], terms[1::2])] + terms[len(terms) // 2 * 2 :]
        return jnp.broadcast_to(jnp.sum(terms[0], axis=1, keepdims=True), (SUB, LANES))

    def weights():
        return [jnp.broadcast_to(rho[k : k + 1, :], (SUB, LANES)) for k in range(chunks)]

    blocks = groups // GROUP

    def swap(slot):
        return pltpu.make_async_remote_copy(
            src_ref=part.at[slot], dst_ref=part_in.at[slot], send_sem=x_send.at[slot], recv_sem=x_recv.at[slot],
            device_id=(mate, g), device_id_type=MESH)

    def iteration(t, low):
        low_s, low_r = low
        slot = lax.rem(t, 2)
        ws = weights()

        def sums(i):
            return [row_sum(i * GROUP + h, ws) for h in range(GROUP)]

        def spread(i, tot, acc, low):
            acc = list(acc)
            for h in range(GROUP):
                r = i * GROUP + h
                low = jnp.minimum(low, tot[h])
                w = bvec[pl.ds(pl.multiple_of(r * SUB, SUB), SUB), :] / tot[h]
                for k in range(chunks):
                    acc[k] = acc[k] + expo[r, k] * w
            return tuple(acc), low

        def body(i, carry):
            tot, acc, low = carry
            fresh = sums(i)
            acc, low = spread(i - 1, tot, acc, low)
            return tuple(fresh), acc, low

        zero = jnp.zeros((SUB, LANES), jnp.float32)
        tot, acc, low_r = lax.fori_loop(1, blocks, body, (tuple(sums(0)), (zero,) * chunks, low_r))
        acc, low_r = spread(blocks - 1, tot, acc, low_r)
        mine = jnp.concatenate([jnp.sum(x, axis=0, keepdims=True) for x in acc], axis=0) * scale[...]
        part[slot, 0:chunks, :] = mine
        part[slot, chunks : chunks + SUB, :] = low_r
        swap(slot).start()
        swap(slot).wait_recv()
        total = mine + part_in[slot, 0:chunks, :]
        low_r = jnp.minimum(low_r, part_in[slot, chunks : chunks + SUB, :])
        low_s = jnp.minimum(low_s, total)
        rho[...] = scale[...] * (mass_a[...] / total)
        tops_now = tops[...] + log2(total)
        own[...] = tops_now
        swap(slot).wait_send()
        return low_s, low_r

    low_s, low_r = lax.fori_loop(
        1, ITERS, iteration,
        (jnp.full((chunks, LANES), 1.0, jnp.float32), jnp.full((SUB, LANES), 1.0, jnp.float32)))

    def wait_hand(i, _):
        s = slot_of(2 * (i // grp_n) + core, i % grp_n)
        o = slot_of(2 * (i // grp_n) + 1 - core, i % grp_n)
        t_push(s, 0).wait_send()
        t_arrive(o)
        return 0

    ws = weights()
    base = ((b // 2) * grp_n + g) * (count // SUB)
    per = count // SUB
    tot = [row_sum(base + h, ws) for h in range(per)]
    for h in range(per):
        low_r = jnp.minimum(low_r, tot[h])
    mine = pl.ds(pl.multiple_of(base * SUB, count), count)
    g_col = (1.0 / ALPHA) * (log2(bvec[mine, :]) - log2(jnp.concatenate(tot, axis=0)))

    def to_lanes(column):
        return jnp.sum(jnp.where(eye, column, 0.0), axis=0, keepdims=True)

    src = src_ref[...]
    square = jnp.sum(src * src, axis=1, keepdims=True)
    eye2 = (lax.broadcasted_iota(jnp.int32, (count, LANES), 1) % count
            == lax.broadcasted_iota(jnp.int32, (count, LANES), 0))
    norm = jnp.sum(jnp.where(eye2, square, 0.0), axis=0, keepdims=True)
    full = norm - (1.0 / ALPHA) * own[pl.ds(me // rep, 1), :]
    picked = full[:, 0:count]
    for i in range(1, rep):
        picked = jnp.where(me % rep == i, full[:, i * count : (i + 1) * count], picked)
    out_ref[0:1, 0:count] = picked
    out_ref[1:2, 0:count] = to_lanes(g_col)[:, 0:count]
    least = jnp.minimum(jnp.min(low_s, axis=0, keepdims=True), jnp.min(low_r, axis=0, keepdims=True))
    out_ref[2:3, :] = least

    lax.fori_loop(0, slots_t, wait_hand, 0)
    copy_t = pltpu.make_async_copy(tgt_all, tgt_hbm, h_sem.at[1])
    copy_t.start()

    def sent_line(step, _):
        line(tpack, tgt_all, t_send, t_recv, step).wait_send()
        line(spack, src_all, s_send, s_recv, step).wait_send()
        return 0

    lax.fori_loop(1, grp_n, sent_line, 0)
    for way in (1, 2):
        first(tpack, tgt_all, g_send, t_recv, way).wait_send()
    for way in (0, 1, 2):
        first(spack, src_all, f_send, s_recv, way).wait_send()

    def sent(pushes, bits, ways, lo, hi):
        def go(step, _):
            for way in ways:
                pushes(slot_of(side(bits), mix(g, step, grp_n)), way).wait_send()
            return 0
        lax.fori_loop(lo, hi, go, 0)

    sent(t_push, 0, (1, 2), 1, grp_n)
    sent(s_push, 0, (1, 2, 0), 1, grp_n)
    sent(t_push, 2, (2,), 0, half)
    sent(t_push, 4, (1,), half, grp_n)
    sent(s_push, 2, (2, 0), 0, half)
    sent(s_push, 4, (0,), 0, half)
    sent(s_push, 4, (1, 0), half, grp_n)
    sent(s_push, 2, (0,), half, grp_n)
    sent(s_push, 6, (0,), 0, grp_n)
    copy_s.wait()
    copy_t.wait()


def safe_kernel(grp_n, count, src_ref, tgt_ref, fast_ref, src_hbm, tgt_hbm, s_out, t_out,
                raw_s, raw_t, src_all, tgt_all, cost, tcat, logb, u, v, loga, sems):
    n_dev = src_all.shape[0]
    points = n_dev * count
    rep = LANES // count
    chunks = points // LANES
    wide = count + 1
    s_out[...] = fast_ref[0:1, 0:count]
    t_out[...] = fast_ref[1:2, 0:count]

    @pl.when(jnp.logical_not(jnp.min(fast_ref[2:3, :]) >= FLOOR))
    def _():
        b, g = lax.axis_index("blk"), lax.axis_index("grp")
        me = b * grp_n + g
        copies = [pltpu.make_async_copy(x, y, sems.at[i]) for i, (x, y) in enumerate(
            [(src_hbm, src_all), (tgt_hbm, tgt_all), (src_ref, raw_s), (tgt_ref, raw_t)])]
        for c in copies:
            c.start()
        for c in copies:
            c.wait()
        eye = (lax.broadcasted_iota(jnp.int32, (count, LANES), 1) % count
               == lax.broadcasted_iota(jnp.int32, (count, LANES), 0))
        low = lax.broadcasted_iota(jnp.int32, (count, LANES), 1) < count

        def target(r, _):
            rows = pl.ds(pl.multiple_of(r * count, count), count)
            block = tgt_all[r, 0:count, :]
            tcat[rows, :] = block
            mass = jnp.sum(jnp.where(eye & low, tgt_all[r, count:wide, :], 0.0), axis=1, keepdims=True)
            square = jnp.sum(block * block, axis=1, keepdims=True)
            mass = log2(jnp.broadcast_to(mass, (count, LANES)))
            logb[rows, :] = mass
            u[rows, :] = mass - ALPHA * square
            return 0

        lax.fori_loop(0, n_dev, target, 0)

        def make_cost(k, _):
            blocks = [src_all[k * rep + i, 0:count, :] for i in range(rep)]
            loga[pl.ds(k, 1), :] = log2(sum(src_all[k * rep + i, count:wide, :] for i in range(rep)))
            s = jnp.concatenate(blocks, axis=0) * (2.0 * ALPHA)

            def rows_of(i, _):
                rows = pl.ds(pl.multiple_of(i * LANES, LANES), LANES)
                cost[k, rows, :] = lax.dot_general(
                    tcat[rows, :], s, (((1,), (1,)), ((), ())),
                    precision=lax.Precision.HIGHEST, preferred_element_type=jnp.float32)
                return 0

            return lax.fori_loop(0, points // LANES, rows_of, 0)

        lax.fori_loop(0, chunks, make_cost, 0)

        def source_step(k, _):
            def block(i, carry):
                m0, s0 = carry
                rows = pl.ds(pl.multiple_of(i * LANES, LANES), LANES)
                x = (cost[k, rows, :] + u[rows, :]).reshape(LANES // SUB, SUB, LANES)
                m = jnp.maximum(m0, jnp.max(x, axis=0))
                return m, s0 * exp2(m0 - m) + jnp.sum(exp2(x - m[None]), axis=0)

            m, s = lax.fori_loop(0, points // LANES, block, (
                jnp.full((SUB, LANES), -1e30, jnp.float32), jnp.zeros((SUB, LANES), jnp.float32)))
            top = jnp.max(m, axis=0, keepdims=True)
            total = jnp.sum(s * exp2(m - top), axis=0, keepdims=True)
            v[pl.ds(k, 1), :] = loga[pl.ds(k, 1), :] - (top + log2(total))
            return 0

        def target_step(r, _):
            rows = pl.ds(pl.multiple_of(r * SUB, SUB), SUB)
            x = [cost[k, rows, :] + v[k : k + 1, :] for k in range(chunks)]
            m = functools.reduce(jnp.maximum, x)
            s = sum(exp2(y - m) for y in x)
            top = jnp.max(m, axis=1, keepdims=True)
            total = jnp.sum(s * exp2(m - top), axis=1, keepdims=True)
            u[rows, :] = logb[rows, :] - (top + log2(total))
            return 0

        def iteration(t, _):
            lax.fori_loop(0, chunks, source_step, 0)
            lax.fori_loop(0, points // SUB, target_step, 0)
            return 0

        lax.fori_loop(0, ITERS, iteration, 0)

        def to_lanes(column):
            return jnp.sum(jnp.where(eye, column, 0.0), axis=0, keepdims=True)

        src = raw_s[...]
        row = pl.ds(me // rep, 1)
        full = to_lanes(jnp.sum(src * src, axis=1, keepdims=True)) - (1.0 / ALPHA) * (loga[row, :] - v[row, :])
        tgt = raw_t[...]
        mine = pl.ds(pl.multiple_of(me * count, count), count)
        second = to_lanes(jnp.sum(tgt * tgt, axis=1, keepdims=True) - (1.0 / ALPHA) * (logb[mine, :] - u[mine, :]))
        picked = full[:, 0:count]
        for i in range(1, rep):
            picked = jnp.where(me % rep == i, full[:, i * count : (i + 1) * count], picked)
        s_out[...] = picked
        t_out[...] = second[:, 0:count]


def fits(blk_n, grp_n, shape):
    count, width = shape
    points = blk_n * grp_n * count
    return (blk_n == OCT and width == LANES and LANES % count == 0 and count % SUB == 0
            and grp_n & (grp_n - 1) == 0 and grp_n > 1 and (grp_n * count) % LANES == 0
            and (points // 2) % (MROWS * GROUP // SUB) == 0 and points * points * 4 <= BUDGET)


def chip_device(blk_n, grp_n, source, target, source_mass, target_mass):
    count = source.shape[0]
    n_dev = blk_n * grp_n
    points = n_dev * count
    nt = points // 2
    chunks = points // LANES
    halves = grp_n * count // LANES
    wide = count + 1
    f32 = jnp.float32
    vmem = pl.BlockSpec(memory_space=pltpu.VMEM)
    hbm = pl.BlockSpec(memory_space=pl.ANY)
    dma = pltpu.SemaphoreType.DMA
    everything = jax.ShapeDtypeStruct((n_dev, wide, LANES), f32)
    fast, src_hbm, tgt_hbm = pl.pallas_call(
        functools.partial(chip_kernel, grp_n, count),
        out_shape=(jax.ShapeDtypeStruct((SUB, LANES), f32), everything, everything),
        in_specs=[vmem] * 4,
        out_specs=(vmem, hbm, hbm),
        scratch_shapes=[
            pltpu.VMEM((n_dev, wide, LANES), f32),
            pltpu.VMEM((n_dev, wide, LANES), f32),
            pltpu.VMEM((wide, LANES), f32),
            pltpu.VMEM((wide, LANES), f32),
            pltpu.VMEM((nt, 2 * LANES), jnp.bfloat16),
            pltpu.VMEM((nt // SUB, chunks, SUB, LANES), f32),
            pltpu.VMEM((nt, LANES), f32),
            pltpu.VMEM((nt, LANES), f32),
            pltpu.VMEM((chunks, LANES), f32),
            pltpu.VMEM((blk_n, 2 * halves, LANES), f32),
            pltpu.VMEM((blk_n, 2 * halves, LANES), f32),
            pltpu.VMEM((2, chunks + SUB, LANES), f32),
            pltpu.VMEM((2, chunks + SUB, LANES), f32),
            pltpu.VMEM((chunks, LANES), f32),
            pltpu.VMEM((chunks, LANES), f32),
            pltpu.VMEM((chunks, LANES), f32),
            pltpu.VMEM((chunks, LANES), f32),
            dma((grp_n,)), dma((3, n_dev)), dma((n_dev,)),
            dma((grp_n,)), dma((3, n_dev)), dma((n_dev,)),
            dma((blk_n,)), dma((blk_n,)), dma((2,)), dma((2,)), dma((2,)),
        ],
        compiler_params=pltpu.CompilerParams(
            collective_id=0, has_side_effects=True, vmem_limit_bytes=62 * 2**20),
    )(source, target, source_mass.reshape(1, count), target_mass.reshape(1, count))
    row = jax.ShapeDtypeStruct((1, count), f32)
    first, second = pl.pallas_call(
        functools.partial(safe_kernel, grp_n, count),
        out_shape=(row, row),
        in_specs=[hbm, hbm, vmem, hbm, hbm],
        out_specs=(vmem, vmem),
        scratch_shapes=[
            pltpu.VMEM((count, LANES), f32),
            pltpu.VMEM((count, LANES), f32),
            pltpu.VMEM((n_dev, wide, LANES), f32),
            pltpu.VMEM((n_dev, wide, LANES), f32),
            pltpu.VMEM((chunks, points, LANES), f32),
            pltpu.VMEM((points, LANES), f32),
            pltpu.VMEM((points, LANES), f32),
            pltpu.VMEM((points, LANES), f32),
            pltpu.VMEM((chunks, LANES), f32),
            pltpu.VMEM((chunks, LANES), f32),
            dma((4,)),
        ],
        compiler_params=pltpu.CompilerParams(vmem_limit_bytes=62 * 2**20),
    )(source, target, fast, src_hbm, tgt_hbm)
    return first.reshape(count), second.reshape(count)


def solution(mesh):
    blk_n, grp_n = mesh.shape["blk"], mesh.shape["grp"]
    n_dev = blk_n * grp_n

    def wide_device(source, target, source_mass, target_mass):
        count, width = source.shape
        points = n_dev * count
        part = OCT
        while part < blk_n and (points // part) * points * 4 > BUDGET:
            part *= 2
        nj = points // part
        t_dev = n_dev // part
        chunks = points // LANES
        pieces = math.gcd(chunks, PIECES)
        wide = count + SUB
        f32 = jnp.float32
        vmem = pl.BlockSpec(memory_space=pltpu.VMEM)
        dma = pltpu.SemaphoreType.DMA
        out = pl.pallas_call(
            functools.partial(wide_kernel, blk_n, grp_n, part, count, pieces),
            out_shape=jax.ShapeDtypeStruct((2, count), f32),
            in_specs=[vmem] * 4,
            out_specs=vmem,
            scratch_shapes=[
                pltpu.VMEM((n_dev, wide, width), f32),
                pltpu.VMEM((t_dev, wide, width), f32),
                pltpu.VMEM((wide, width), f32),
                pltpu.VMEM((wide, width), f32),
                pltpu.VMEM((chunks, nj, LANES), f32),
                pltpu.VMEM((nj, width), f32),
                pltpu.VMEM((nj, LANES), f32),
                pltpu.VMEM((chunks, LANES), f32),
                pltpu.VMEM((chunks, LANES), f32),
                pltpu.VMEM((nj, LANES), f32),
                pltpu.VMEM((2, pieces, part, chunks // pieces, LANES), f32),
                pltpu.VMEM((pieces, nj, LANES), f32),
                pltpu.VMEM((pieces, nj, LANES), f32),
                dma((n_dev // OCT,)), dma((3, n_dev)), dma((n_dev,)),
                dma((t_dev,)), dma((t_dev,)),
                dma((2, pieces, part)), dma((2, pieces, part)),
            ],
            compiler_params=pltpu.CompilerParams(
                collective_id=0, has_side_effects=True, vmem_limit_bytes=62 * 2**20),
        )(source, target, source_mass.reshape(1, count), target_mass.reshape(1, count))
        return out[0], out[1]

    def per_device(source, target, source_mass, target_mass):
        if fits(blk_n, grp_n, source.shape):
            return chip_device(blk_n, grp_n, source, target, source_mass, target_mass)
        return wide_device(source, target, source_mass, target_mass)

    both = P(("blk", "grp"))
    return jax.shard_map(
        per_device,
        mesh=mesh,
        in_specs=(P(("blk", "grp"), None), P(("blk", "grp"), None), both, both),
        out_specs=(both, both),
        check_vma=False,
    )
```
